32 devices in a mesh: groups: 2 (over y), seq: 4 (over z), batch: 4 (over x, core).
Axes of the slice: x: 2, y: 2, z: 4, core: 2. Of those that a mesh axis runs over, the one named last changes fastest.
Arguments:
- queries: bfloat16 [8, 512, 2048], P(('groups', 'batch'), 'seq'), parts along dimension 0, may hold values from -80 to 80, as said below
- keys: bfloat16 [8, 512, 512], P(('groups', 'batch'), 'seq'), parts along dimension 0, may hold values from -4.5 to 4.5
- values: bfloat16 [8, 512, 512], P(('groups', 'batch'), 'seq'), parts along dimension 0, may hold values from -6 to 6
Outputs:
- attended: bfloat16 [8, 512, 2048], P(('groups', 'batch'), 'seq'), parts along dimension 0
The draws below stay inside these ranges and needn't reach their ends.
There are 2 independent parts, one for each index of `groups`. The reference program is written for one: setup_inputs(seed, part) draws one part's arguments, and reference() takes and returns one part's arrays. A program takes and returns all parts, laid end to end along the dimension named above; each array names one. Nothing has to cross between parts.
Inputs may be any that keep to these rules, and one draw needn't show every extreme that they name: `queries`: query vectors of order a few units; a few positions may hold much larger entries.
All inputs are finite; a program needn't handle non-finite values.
Results may differ from the reference program's by a relative error of at most 0.009.
Values may be sent and summed in bfloat16 or wider, within the bound.
A program may use at most 64 MiB of HBM per device.

```python
import math
import jax
import jax.numpy as jnp
from jax import lax

QUERY_HEADS = 16
KEY_VALUE_HEADS = 4
HEAD_SIZE = 128
SEQUENCE_LENGTH = 512
GROUP_SEQUENCES = 4


def plant_plan(key):
    start_offset = jnp.clip(jax.random.normal(jax.random.fold_in(key, 1), (GROUP_SEQUENCES, SEQUENCE_LENGTH, KEY_VALUE_HEADS * HEAD_SIZE), jnp.float32), -4.5, 4.5)
    return start_offset


def draw_keys(key, part):
    start_offset = plant_plan(key)
    return start_offset.astype(jnp.bfloat16)


def draw_queries(key, part):
    return jnp.clip(2.0 * jax.random.normal(jax.random.fold_in(key, 5), (GROUP_SEQUENCES, SEQUENCE_LENGTH, QUERY_HEADS * HEAD_SIZE), jnp.float32), -12.0, 12.0).astype(jnp.bfloat16)


def block_levels(key, extent, pieces, low, top_value):
    factor_of, own = 1.0, jax.random.fold_in(key, 6)
    for axis_at, parts in pieces:
        draws = jnp.exp(jax.random.uniform(jax.random.fold_in(own, axis_at), (parts,), jnp.float32, low / len(pieces), top_value / len(pieces)))
        factor_of = factor_of * jnp.repeat(draws, extent[axis_at] // parts).reshape([-1 if axis == axis_at else 1 for axis in range(len(extent))])
    return factor_of


def scatter_about(stream_key, dims, scale, reach, shards=(), kind=jnp.bfloat16):
    gain = block_levels(stream_key, dims, shards, -0.22, 0.18) if shards else 1.0
    drawn = jax.random.normal(stream_key, dims, jnp.float32) * scale * gain
    return jnp.minimum(jnp.maximum(drawn, -reach), reach).astype(kind)


def setup_inputs(seed: int = 0, part: int = 0) -> dict:
    seeds = jax.random.split(jax.random.key(seed), 4)
    own_keys = jax.random.split(jax.random.fold_in(seeds[3], part), 4)
    queries = draw_queries(jax.random.fold_in(jax.random.fold_in(seeds[3], part), 71), part)
    keys = draw_keys(jax.random.fold_in(jax.random.fold_in(seeds[3], part), 71), part)
    values = scatter_about(own_keys[2], (GROUP_SEQUENCES, SEQUENCE_LENGTH, KEY_VALUE_HEADS * HEAD_SIZE), 1.0, 6.0, ((0, 4), (1, 4)))
    return {"queries": queries, "keys": keys, "values": values}


def attend_block(rows_of_query, start, keys_single_float, values_single_float):
    rows_per_block = rows_of_query.shape[0]
    query_heads_per_group = QUERY_HEADS // KEY_VALUE_HEADS
    query_single_float = rows_of_query.astype(jnp.float32).reshape(rows_per_block, KEY_VALUE_HEADS, query_heads_per_group, HEAD_SIZE)
    scores = jnp.einsum('qkgd,pkd->qkgp', query_single_float, keys_single_float) / math.sqrt(HEAD_SIZE)
    row_pos = start + jnp.arange(rows_per_block, dtype=jnp.int32)
    key_pos = jnp.arange(SEQUENCE_LENGTH, dtype=jnp.int32)
    visible = (key_pos[None, :] <= row_pos[:, None])[:, None, None, :]
    scores = jnp.where(visible, scores, -jnp.inf)
    weights = jax.nn.softmax(scores, axis=-1).astype(jnp.bfloat16)
    mixed = jnp.einsum('qkgp,pkd->qkgd', weights.astype(jnp.float32), values_single_float)
    return mixed.reshape(rows_per_block, QUERY_HEADS * HEAD_SIZE).astype(jnp.bfloat16)

def one_sequence(operands):
    seq_queries, sequence_keys, sequence_values = operands
    keys_single_float = sequence_keys.astype(jnp.float32).reshape(SEQUENCE_LENGTH, KEY_VALUE_HEADS, HEAD_SIZE)
    values_single_float = sequence_values.astype(jnp.float32).reshape(SEQUENCE_LENGTH, KEY_VALUE_HEADS, HEAD_SIZE)
    rows_per_block = min(512, SEQUENCE_LENGTH)
    num_blocks = SEQUENCE_LENGTH // rows_per_block
    query_blocks = seq_queries.reshape(num_blocks, rows_per_block, QUERY_HEADS * HEAD_SIZE)
    starts = jnp.arange(num_blocks, dtype=jnp.int32) * rows_per_block

    def visit_block(block_args):
        return attend_block(block_args[0], block_args[1], keys_single_float, values_single_float)
    outputs = lax.map(visit_block, (query_blocks, starts))
    return outputs.reshape(SEQUENCE_LENGTH, QUERY_HEADS * HEAD_SIZE)

def reference(queries, keys, values):
    return lax.map(one_sequence, (queries, keys, values))
```

```python
import functools
import math

import jax
import jax.numpy as jnp
from jax import lax
from jax.experimental import pallas as pl
from jax.experimental.pallas import tpu as pltpu
from jax.sharding import PartitionSpec as P

HEAD_SIZE = 128
SCALE = math.log2(math.e) / math.sqrt(HEAD_SIZE)
MESH = pl.DeviceIdType.MESH


def kernel(
    n, groups, per_group,
    q_hbm, k_hbm, v_hbm, o_hbm,
    q, kv, m, acc, o,
    load_sem, q_sem, o_sem, send_sem, recv_sem,
):
    rows = q.shape[0]
    me = lax.axis_index("seq")
    right, left = lax.rem(me + 1, n), lax.rem(me + n - 1, n)
    wide = per_group * HEAD_SIZE

    def loads(g):
        cols = pl.ds(g * HEAD_SIZE, HEAD_SIZE)
        return (
            pltpu.make_async_copy(
                k_hbm.at[0, :, cols], kv.at[0, g, pl.ds(0, rows)], load_sem.at[0, g]
            ),
            pltpu.make_async_copy(
                v_hbm.at[0, :, cols], kv.at[0, g, pl.ds(rows, rows)], load_sem.at[1, g]
            ),
        )

    def send(slot, g):
        return pltpu.make_async_remote_copy(
            src_ref=kv.at[slot, g],
            dst_ref=kv.at[slot + 1, g],
            send_sem=send_sem.at[slot, g],
            recv_sem=recv_sem.at[slot + 1, g],
            device_id={"seq": right},
            device_id_type=MESH,
        )

    def receive(slot, g):
        return pltpu.make_async_remote_copy(
            src_ref=kv.at[slot, g],
            dst_ref=kv.at[slot, g],
            send_sem=send_sem.at[slot, g],
            recv_sem=recv_sem.at[slot, g],
            device_id={"seq": right},
            device_id_type=MESH,
        )

    def out_copy(g):
        cols = pl.ds(g * wide, wide)
        return pltpu.make_async_copy(o.at[:, cols], o_hbm.at[0, :, cols], o_sem.at[g])

    q_copy = pltpu.make_async_copy(q_hbm.at[0], q, q_sem)

    barrier = pltpu.get_barrier_semaphore()

    @pl.when(me > 0)
    def _():
        pl.semaphore_signal(barrier, inc=1, device_id={"seq": left}, device_id_type=MESH)

    for g in range(groups):
        for copy in loads(g):
            copy.start()
    q_copy.start()

    @pl.when(me < n - 1)
    def _():
        pl.semaphore_wait(barrier, 1)

    for g in range(groups):
        for copy in loads(g):
            copy.wait()

        @pl.when(me < n - 1)
        def _():
            send(0, g).start()

    q_copy.wait()

    def scores_of(slot, g):
        stacked = jnp.concatenate(
            [
                q[:, (g * per_group + h) * HEAD_SIZE : (g * per_group + h + 1) * HEAD_SIZE]
                for h in range(per_group)
            ],
            axis=0,
        )
        return lax.dot_general(
            stacked,
            kv[slot, g, :rows, :],
            (((1,), (1,)), ((), ())),
            preferred_element_type=jnp.float32,
        )

    def weighted(p, slot, g):
        block = jnp.concatenate(
            [kv[slot, g, rows:, :], jnp.ones((rows, HEAD_SIZE), jnp.bfloat16)], axis=1
        )
        return jnp.dot(p.astype(jnp.bfloat16), block, preferred_element_type=jnp.float32)

    def finish(total, g):
        done = (total[:, :HEAD_SIZE] / total[:, HEAD_SIZE:]).astype(jnp.bfloat16)
        for h in range(per_group):
            at = (g * per_group + h) * HEAD_SIZE
            o[:, at : at + HEAD_SIZE] = done[h * rows : (h + 1) * rows]
        out_copy(g).start()

    row = lax.rem(lax.broadcasted_iota(jnp.int32, (per_group * rows, rows), 0), rows)
    visible = lax.broadcasted_iota(jnp.int32, (per_group * rows, rows), 1) <= row

    for g in range(groups):
        s = jnp.where(visible, scores_of(0, g), -1e30)
        new_m = jnp.max(s, axis=1, keepdims=True)
        total = weighted(jnp.exp2((s - new_m) * SCALE), 0, g)
        acc[g] = total
        m[g] = jnp.broadcast_to(new_m, m.shape[1:])

        @pl.when(me == 0)
        def _():
            finish(acc[g], g)

    @pl.loop(1, me + 1)
    def _(slot):
        for g in range(groups):
            receive(slot, g).wait_recv()

            @pl.when(me < n - 1)
            def _():
                send(slot, g).start()

            s = scores_of(slot, g)
            old_m = m[g]
            new_m = jnp.maximum(old_m, jnp.max(s, axis=1, keepdims=True))
            fade = jnp.exp2((old_m - new_m) * SCALE)
            p = jnp.exp2((s - new_m[:, :1]) * SCALE)
            total = acc[g] * jnp.concatenate([fade, fade], axis=1) + weighted(p, slot, g)

            @pl.when(slot < me)
            def _():
                acc[g] = total
                m[g] = new_m

            @pl.when(slot == me)
            def _():
                finish(total, g)

    @pl.when(me < n - 1)
    def _():
        @pl.loop(0, me + 1)
        def _(slot):
            for g in range(groups):
                send(slot, g).wait_send()

    for g in range(groups):
        out_copy(g).wait()


def on_device(n, queries, keys, values):
    rows, query_width = queries.shape[1:]
    groups = keys.shape[2] // HEAD_SIZE
    per_group = query_width // HEAD_SIZE // groups
    hbm = pl.BlockSpec(memory_space=pl.ANY)
    return pl.pallas_call(
        functools.partial(kernel, n, groups, per_group),
        out_shape=jax.ShapeDtypeStruct(queries.shape, queries.dtype),
        in_specs=[hbm, hbm, hbm],
        out_specs=hbm,
        scratch_shapes=[
            pltpu.VMEM((rows, query_width), jnp.bfloat16),
            pltpu.VMEM((n, groups, 2 * rows, HEAD_SIZE), jnp.bfloat16),
            pltpu.VMEM((groups, per_group * rows, HEAD_SIZE), jnp.float32),
            pltpu.VMEM((groups, per_group * rows, 2 * HEAD_SIZE), jnp.float32),
            pltpu.VMEM((rows, query_width), jnp.bfloat16),
            pltpu.SemaphoreType.DMA((2, groups)),
            pltpu.SemaphoreType.DMA,
            pltpu.SemaphoreType.DMA((groups,)),
            pltpu.SemaphoreType.DMA((n, groups)),
            pltpu.SemaphoreType.DMA((n, groups)),
        ],
        compiler_params=pltpu.CompilerParams(collective_id=0, has_side_effects=True),
    )(queries, keys, values)


def solution(mesh):
    spec = P(("groups", "batch"), "seq", None)
    return jax.shard_map(
        functools.partial(on_device, mesh.shape["seq"]),
        mesh=mesh,
        in_specs=(spec, spec, spec),
        out_specs=spec,
        check_vma=False,
    )
```

```python
import functools
import math

import jax
import jax.numpy as jnp
from jax import lax
from jax.experimental import pallas as pl
from jax.experimental.pallas import tpu as pltpu
from jax.sharding import PartitionSpec as P

HEAD_SIZE = 128
SCALE = math.log2(math.e) / math.sqrt(HEAD_SIZE)
MESH = pl.DeviceIdType.MESH


def kernel(
    n, groups, per_group,
    q_hbm, k_hbm, v_hbm, o,
    q, kv, m, acc,
    load_sem, q_sem, send_sem, recv_sem,
):
    rows = q.shape[0]
    me = lax.axis_index("seq")
    right, left = lax.rem(me + 1, n), lax.rem(me + n - 1, n)

    def loads(g):
        cols = pl.ds(g * HEAD_SIZE, HEAD_SIZE)
        return (
            pltpu.make_async_copy(
                k_hbm.at[0, :, cols], kv.at[0, g, pl.ds(0, rows)], load_sem.at[0, g]
            ),
            pltpu.make_async_copy(
                v_hbm.at[0, :, cols], kv.at[0, g, pl.ds(rows, rows)], load_sem.at[1, g]
            ),
        )

    def send(slot, g):
        return pltpu.make_async_remote_copy(
            src_ref=kv.at[slot, g],
            dst_ref=kv.at[slot + 1, g],
            send_sem=send_sem.at[slot, g],
            recv_sem=recv_sem.at[slot + 1, g],
            device_id={"seq": right},
            device_id_type=MESH,
        )

    def receive(slot, g):
        return pltpu.make_async_remote_copy(
            src_ref=kv.at[slot, g],
            dst_ref=kv.at[slot, g],
            send_sem=send_sem.at[slot, g],
            recv_sem=recv_sem.at[slot, g],
            device_id={"seq": right},
            device_id_type=MESH,
        )

    q_copy = pltpu.make_async_copy(q_hbm.at[0], q, q_sem)

    barrier = pltpu.get_barrier_semaphore()

    @pl.when(me > 0)
    def _():
        pl.semaphore_signal(barrier, inc=1, device_id={"seq": left}, device_id_type=MESH)

    for g in range(groups):
        for copy in loads(g):
            copy.start()
    q_copy.start()

    @pl.when(me < n - 1)
    def _():
        pl.semaphore_wait(barrier, 1)

    for g in range(groups):
        for copy in loads(g):
            copy.wait()

        @pl.when(me < n - 1)
        def _():
            send(0, g).start()

    q_copy.wait()

    def scores_of(slot, g):
        stacked = jnp.concatenate(
            [
                q[:, (g * per_group + h) * HEAD_SIZE : (g * per_group + h + 1) * HEAD_SIZE]
                for h in range(per_group)
            ],
            axis=0,
        )
        return lax.dot_general(
            stacked,
            kv[slot, g, :rows, :],
            (((1,), (1,)), ((), ())),
            preferred_element_type=jnp.float32,
        )

    def weighted(p, slot, g):
        block = jnp.concatenate(
            [kv[slot, g, rows:, :], jnp.ones((rows, HEAD_SIZE), jnp.bfloat16)], axis=1
        )
        return jnp.dot(p.astype(jnp.bfloat16), block, preferred_element_type=jnp.float32)

    def finish(total, g):
        done = (total[:, :HEAD_SIZE] / total[:, HEAD_SIZE:]).astype(jnp.bfloat16)
        for h in range(per_group):
            at = (g * per_group + h) * HEAD_SIZE
            o[0, :, at : at + HEAD_SIZE] = done[h * rows : (h + 1) * rows]

    row = lax.rem(lax.broadcasted_iota(jnp.int32, (per_group * rows, rows), 0), rows)
    visible = lax.broadcasted_iota(jnp.int32, (per_group * rows, rows), 1) <= row

    for g in range(groups):
        s = jnp.where(visible, scores_of(0, g), -1e30)
        new_m = jnp.max(s, axis=1, keepdims=True)
        total = weighted(jnp.exp2((s - new_m) * SCALE), 0, g)
        acc[g] = total
        m[g] = jnp.broadcast_to(new_m, m.shape[1:])

        @pl.when(me == 0)
        def _():
            finish(acc[g], g)

    @pl.loop(1, me + 1)
    def _(slot):
        for g in range(groups):
            receive(slot, g).wait_recv()

            @pl.when(me < n - 1)
            def _():
                send(slot, g).start()

            s = scores_of(slot, g)
            old_m = m[g]
            new_m = jnp.maximum(old_m, jnp.max(s, axis=1, keepdims=True))
            fade = jnp.exp2((old_m - new_m) * SCALE)
            p = jnp.exp2((s - new_m[:, :1]) * SCALE)
            total = acc[g] * jnp.concatenate([fade, fade], axis=1) + weighted(p, slot, g)

            @pl.when(slot < me)
            def _():
                acc[g] = total
                m[g] = new_m

            @pl.when(slot == me)
            def _():
                finish(total, g)

    @pl.when(me < n - 1)
    def _():
        @pl.loop(0, me + 1)
        def _(slot):
            for g in range(groups):
                send(slot, g).wait_send()


def on_device(n, queries, keys, values):
    rows, query_width = queries.shape[1:]
    groups = keys.shape[2] // HEAD_SIZE
    per_group = query_width // HEAD_SIZE // groups
    hbm = pl.BlockSpec(memory_space=pltpu.HBM)
    held = (2 * rows * query_width + 2 * n * rows * keys.shape[2]) * 2 + 3 * rows * query_width * 4
    return pl.pallas_call(
        functools.partial(kernel, n, groups, per_group),
        out_shape=jax.ShapeDtypeStruct(queries.shape, queries.dtype),
        in_specs=[hbm, hbm, hbm],
        out_specs=pl.BlockSpec(memory_space=pltpu.VMEM),
        scratch_shapes=[
            pltpu.VMEM((rows, query_width), jnp.bfloat16),
            pltpu.VMEM((n, groups, 2 * rows, HEAD_SIZE), jnp.bfloat16),
            pltpu.VMEM((groups, per_group * rows, HEAD_SIZE), jnp.float32),
            pltpu.VMEM((groups, per_group * rows, 2 * HEAD_SIZE), jnp.float32),
            pltpu.SemaphoreType.DMA((2, groups)),
            pltpu.SemaphoreType.DMA,
            pltpu.SemaphoreType.DMA((n, groups)),
            pltpu.SemaphoreType.DMA((n, groups)),
        ],
        compiler_params=pltpu.CompilerParams(collective_id=0, has_side_effects=True, vmem_limit_bytes=held + 4 * 2**20),
    )(*(pltpu.with_memory_space_constraint(x, pltpu.HBM) for x in (queries, keys, values)))


def solution(mesh):
    spec = P(("groups", "batch"), "seq", None)
    return jax.shard_map(
        functools.partial(on_device, mesh.shape["seq"]),
        mesh=mesh,
        in_specs=(spec, spec, spec),
        out_specs=spec,
        check_vma=False,
    )
```
